128 devices in a mesh: shard: 8 (over y, x_lo), cols: 16 (over z, x_hi, core).
Axes of the slice: x: 4 (x_hi: 2, x_lo: 2; x = x_hi * 2 + x_lo), y: 4, z: 4, core: 2. Of those that a mesh axis runs over, the one named last changes fastest.
Arguments:
- train_gate: bfloat16 [4096, 14336], P('shard', 'cols'), may hold values from -0.09375 to 0.09375
- low_gate: bfloat16 [4096, 32], P('shard'), may hold values from -0.09375 to 0.09375
- high_gate: bfloat16 [32, 14336], P(None, 'cols'), may hold values from -1 to 1
- train_up: bfloat16 [4096, 14336], P('shard', 'cols'), may hold values from -0.09375 to 0.09375
- low_up: bfloat16 [4096, 32], P('shard'), may hold values from -0.09375 to 0.09375
- high_up: bfloat16 [32, 14336], P(None, 'cols'), may hold values from -1 to 1
- norm_train: float32 [4096], P(('shard', 'cols')), may hold values from 0.25 to 1.75
- norm_step: float32 [4096], P(('shard', 'cols')), may hold values from -0.3 to 0.3
Outputs:
- ready_gate: bfloat16 [14336, 4096], P('cols')
- ready_up: bfloat16 [14336, 4096], P('cols')
- serve_norm: bfloat16 [4096], replicated
The draws below stay inside these ranges and needn't reach their ends.
All inputs are finite; a program needn't handle non-finite values.
Results may differ from the reference program's by a relative error of at most 0.001.
Values may be sent and summed in bfloat16 or wider, within the bound.
No kernel may reach another device: no remote copies, remote signals or barrier semaphores. Data moves between devices by JAX's collectives and lax.ppermute only.
A program may use at most 128 MiB of HBM per device.

```python
import jax
import jax.numpy as jnp

D_MODEL = 4096
D_INNER = 14336
RANK = 32


def steps_of(own_key, dims, pieces, smallest, high):
    loudness, own = 1.0, jax.random.fold_in(own_key, 6)
    for axis_at, blocks in pieces:
        draws = jnp.exp(jax.random.uniform(jax.random.fold_in(own, axis_at), (blocks,), jnp.float32, smallest / len(pieces), high / len(pieces)))
        loudness = loudness * jnp.repeat(draws, dims[axis_at] // blocks).reshape([-1 if axis == axis_at else 1 for axis in range(len(dims))])
    return loudness


def scatter_about(rng, shape, scale, bound, cuts=(), held_as=jnp.bfloat16):
    loudness = steps_of(rng, shape, cuts, -0.22, 0.18) if cuts else 1.0
    values = jax.random.normal(rng, shape, jnp.float32) * scale * loudness
    return jnp.minimum(jnp.maximum(values, -bound), bound).astype(held_as)


def setup_inputs(seed: int = 0) -> dict:
    key_list = jax.random.split(jax.random.key(seed), 9)
    return {
        "train_gate": scatter_about(key_list[0], (D_MODEL, D_INNER), D_MODEL ** -0.5, 0.09375, ((0, 8), (1, 16))),
        "low_gate": scatter_about(key_list[1], (D_MODEL, RANK), D_MODEL ** -0.5, 0.09375, ((0, 8),)),
        "high_gate": scatter_about(key_list[2], (RANK, D_INNER), RANK ** -0.5, 1.0, ((1, 16),)),
        "train_up": scatter_about(key_list[3], (D_MODEL, D_INNER), D_MODEL ** -0.5, 0.09375, ((0, 8), (1, 16))),
        "low_up": scatter_about(key_list[4], (D_MODEL, RANK), D_MODEL ** -0.5, 0.09375, ((0, 8),)),
        "high_up": scatter_about(key_list[5], (RANK, D_INNER), RANK ** -0.5, 1.0, ((1, 16),)),
        "norm_train": jnp.clip(1.0 + 0.15 * jax.random.normal(key_list[6], (D_MODEL,), jnp.float32), 0.25, 1.75),
        "norm_step": jnp.clip(jax.random.uniform(key_list[7], (D_MODEL,), jnp.float32, -0.3, 0.3) * steps_of(key_list[7], (D_MODEL,), ((0, 128),), -0.4, 0.0), -0.3, 0.3),
    }


mix_rate = 1.0


def reference(train_gate, low_gate, high_gate, train_up, low_up, high_up, norm_train, norm_step):
    latest_gate = train_gate.astype(jnp.float32) + mix_rate * jnp.dot(low_gate, high_gate, preferred_element_type=jnp.float32)
    latest_up = train_up.astype(jnp.float32) + mix_rate * jnp.dot(low_up, high_up, preferred_element_type=jnp.float32)
    ready_gate = latest_gate.T.astype(jnp.bfloat16)
    ready_up = latest_up.T.astype(jnp.bfloat16)
    serve_norm = (norm_train + norm_step).astype(jnp.bfloat16)
    return ready_gate, ready_up, serve_norm
```

```python
import jax
import jax.numpy as jnp
from jax import lax
from jax.experimental import pallas as pl
from jax.experimental.pallas import tpu as pltpu
from jax.sharding import Mesh
from jax.sharding import PartitionSpec as P


mix_rate = 1.0
LANES = 128
UP = [(i, (i + 1) % 4) for i in range(4)]
DOWN = [(i, (i - 1) % 4) for i in range(4)]
SWAP = [(0, 1), (1, 0)]


def merged(train, low, high):
    wide = train.astype(jnp.float32) + mix_rate * jnp.dot(
        low, high, preferred_element_type=jnp.float32
    )
    return wide.astype(jnp.bfloat16)


def place(outs, parts, starts):
    fresh = not isinstance(outs[0], jax.Array)
    count = len(parts)
    steps = [p.shape[1] // LANES for p, _, _ in parts]

    def kernel(*refs):
        starts_ref, refs = refs[0], refs[1:]
        piece_refs, refs = refs[:count], refs[count:]
        refs = refs[0 if fresh else 2 :]
        out_refs, refs = refs[:2], refs[2:]
        taken, turned = refs[:count], refs[count : 2 * count]
        in_sem, out_sem = refs[2 * count :]

        def load(k, c):
            columns = pl.ds(pl.multiple_of(c * LANES, LANES), LANES)
            return pltpu.make_async_copy(
                piece_refs[k].at[:, columns], taken[k].at[c], in_sem.at[k, c]
            )

        def save(k, c):
            rows = pl.ds(pl.multiple_of(parts[k][2] + c * LANES, LANES), LANES)
            columns = pl.ds(pl.multiple_of(starts_ref[k], LANES), parts[k][0].shape[0])
            return pltpu.make_async_copy(
                turned[k].at[c], out_refs[parts[k][1]].at[rows, columns], out_sem.at[k, c]
            )

        for k in range(count):
            for c in range(steps[k]):
                load(k, c).start()
        for k in range(count):

            @pl.loop(0, steps[k])
            def _(c):
                load(k, c).wait()
                turned[k][c] = taken[k][c].T
                save(k, c).start()

        for k in range(count):
            for c in range(steps[k]):
                save(k, c).wait()

    shapes = [jax.ShapeDtypeStruct(o.shape, o.dtype) for o in outs]
    any_spec = pl.BlockSpec(memory_space=pl.ANY)
    operands = [jnp.stack(starts), *[p for p, _, _ in parts], *([] if fresh else outs)]
    moved = sum(p.size * 2 * 2 for p, _, _ in parts)
    return pl.pallas_call(
        kernel,
        out_shape=shapes,
        in_specs=[pl.BlockSpec(memory_space=pltpu.SMEM)] + [any_spec] * (len(operands) - 1),
        out_specs=[any_spec] * 2,
        scratch_shapes=[
            *[pltpu.VMEM((p.shape[1] // LANES, p.shape[0], LANES), p.dtype) for p, _, _ in parts],
            *[pltpu.VMEM((p.shape[1] // LANES, LANES, p.shape[0]), p.dtype) for p, _, _ in parts],
            pltpu.SemaphoreType.DMA((count, max(steps))),
            pltpu.SemaphoreType.DMA((count, max(steps))),
        ],
        input_output_aliases={} if fresh else {count + 1: 0, count + 2: 1},
        compiler_params=pltpu.CompilerParams(vmem_limit_bytes=32 * 2**20),
        cost_estimate=pl.CostEstimate(flops=0, bytes_accessed=moved, transcendentals=0),
    )(*operands)


def doubled(x, axis, bit):
    size = lax.axis_size(axis)
    other = lax.ppermute(x, axis, [(i, i ^ bit) for i in range(size)])
    high = (lax.axis_index(axis) & bit) != 0
    return jnp.where(high, jnp.concatenate([other, x]), jnp.concatenate([x, other]))


def gathered_gain(gain):
    peers = []
    me = lax.axis_index("y") * 2 + lax.axis_index("xl")
    for bit in range(1, 8):
        pairs = [(i, i ^ bit) for i in range(8)]
        peers.append((me ^ bit, lax.ppermute(gain, ("y", "xl"), pairs)))
    length = gain.shape[0]
    rows = jnp.zeros((8, length), gain.dtype)
    index = jnp.arange(8)[:, None]
    rows = jnp.where(index == me, gain[None], rows)
    for at, part in peers:
        rows = jnp.where(index == at, part[None], rows)
    flat = rows.reshape(-1)
    x = flat.reshape(1, -1)
    for bit in (1, 2, 4, 8):
        x = doubled(x, "cols", bit)
    return jnp.moveaxis(x.reshape(16, 8, length), 0, 1).reshape(-1)


def per_device(train_gate, low_gate, high_gate, train_up, low_up, high_up, norm_train, norm_step):
    rows, width = train_gate.shape
    cut = width * 5 // 7 // LANES * LANES
    y, xl = lax.axis_index("y"), lax.axis_index("xl")

    def column(dy, dx):
        return ((((y + dy) % 4) * 2 + (xl + dx) % 2) * rows).astype(jnp.int32)

    def up(v):
        return lax.ppermute(v, "y", UP)

    def down(v):
        return lax.ppermute(v, "y", DOWN)

    def across(v):
        return lax.ppermute(v, "xl", SWAP)

    g = merged(train_gate, low_gate, high_gate)
    u = merged(train_up, low_up, high_up)
    gain = (norm_train + norm_step).astype(jnp.bfloat16)

    g_m, g_x, u_p = up(g), across(g), down(u)
    u_m, u_x, g_p = up(u), across(u), down(g)
    g_f, cg_p, cu_p = up(g_m), down(g_x), across(u_p)
    cu_m0, cu_m1 = across(u_m[:, :cut]), across(u_m[:, cut:])
    cg_m, u_f = up(g_x), down(u_p)
    cg_f0 = across(g_f[:, :cut])
    cg_f1, cu_f1 = down(cg_p[:, cut:]), down(cu_p[:, cut:])
    cu_f0 = up(cu_m0)

    out = jax.ShapeDtypeStruct((width, rows * 8), jnp.bfloat16)
    outs = place((out, out), [(g, 0, 0), (u, 1, 0)], [column(0, 0)] * 2)
    outs = place(outs, [(g_m, 0, 0), (g_x, 0, 0), (u_p, 1, 0)], [column(-1, 0), column(0, 1), column(1, 0)])
    outs = place(outs, [(u_m, 1, 0), (u_x, 1, 0), (g_p, 0, 0)], [column(-1, 0), column(0, 1), column(1, 0)])
    outs = place(outs, [(g_f, 0, 0), (cg_p, 0, 0), (cu_p, 1, 0)], [column(2, 0), column(1, 1), column(1, 1)])
    outs = place(
        outs,
        [(cu_m0, 1, 0), (cu_m1, 1, cut), (cg_m, 0, 0), (u_f, 1, 0)],
        [column(-1, 1), column(-1, 1), column(-1, 1), column(2, 0)],
    )
    outs = place(
        outs,
        [(cg_f0, 0, 0), (cg_f1, 0, cut), (cu_f0, 1, 0), (cu_f1, 1, cut)],
        [column(2, 1), column(2, 1), column(2, 1), column(2, 1)],
    )
    return (*outs, gathered_gain(gain))


def solution(mesh):
    finer = Mesh(mesh.devices.reshape(4, 2, mesh.shape["cols"]), ("y", "xl", "cols"))
    shard, every = ("y", "xl"), ("y", "xl", "cols")
    return jax.shard_map(
        per_device,
        mesh=finer,
        in_specs=(
            P(shard, "cols"),
            P(shard, None),
            P(None, "cols"),
            P(shard, "cols"),
            P(shard, None),
            P(None, "cols"),
            P(every),
            P(every),
        ),
        out_specs=(P("cols", None), P("cols", None), P()),
        check_vma=False,
    )
```

```python
import jax
import jax.numpy as jnp
from jax import lax
from jax.experimental import pallas as pl
from jax.experimental.pallas import tpu as pltpu
from jax.sharding import Mesh
from jax.sharding import PartitionSpec as P


mix_rate = 1.0
LANES = 128
UP = [(i, (i + 1) % 4) for i in range(4)]
DOWN = [(i, (i - 1) % 4) for i in range(4)]
SWAP = [(0, 1), (1, 0)]


def merged(train, low, high):
    wide = train.astype(jnp.float32) + mix_rate * jnp.dot(
        low, high, preferred_element_type=jnp.float32
    )
    return wide.astype(jnp.bfloat16)


def place(outs, parts):
    fresh = not isinstance(outs[0], jax.Array)
    count = len(parts)
    steps = [p.shape[1] // LANES for p, *_ in parts]

    def kernel(*refs):
        y, xl = lax.axis_index("y"), lax.axis_index("xl")
        piece_refs, refs = refs[:count], refs[count:]
        refs = refs[0 if fresh else 2 :]
        out_refs, refs = refs[:2], refs[2:]
        taken, turned = refs[:count], refs[count : 2 * count]
        in_sem, out_sem = refs[2 * count :]

        def load(k, c):
            columns = pl.ds(pl.multiple_of(c * LANES, LANES), LANES)
            return pltpu.make_async_copy(
                piece_refs[k].at[:, columns], taken[k].at[c], in_sem.at[k, c]
            )

        def save(k, c):
            rows = pl.ds(pl.multiple_of(parts[k][2] + c * LANES, LANES), LANES)
            size = parts[k][0].shape[0]
            source = lax.rem(y + parts[k][3], 4) * 2 + lax.rem(xl + parts[k][4], 2)
            columns = pl.ds(pl.multiple_of(source * size, LANES), size)
            return pltpu.make_async_copy(
                turned[k].at[c], out_refs[parts[k][1]].at[rows, columns], out_sem.at[k, c]
            )

        for k in range(count):
            for c in range(steps[k]):
                load(k, c).start()
        for k in range(count):

            @pl.loop(0, steps[k])
            def _(c):
                load(k, c).wait()
                turned[k][c] = taken[k][c].T
                save(k, c).start()

        for k in range(count):
            for c in range(steps[k]):
                save(k, c).wait()

    shapes = [jax.ShapeDtypeStruct(o.shape, o.dtype) for o in outs]
    any_spec = pl.BlockSpec(memory_space=pl.ANY)
    operands = [*[p for p, *_ in parts], *([] if fresh else outs)]
    moved = sum(p.size * 2 * 2 for p, *_ in parts)
    return pl.pallas_call(
        kernel,
        out_shape=shapes,
        in_specs=[any_spec] * len(operands),
        out_specs=[any_spec] * 2,
        scratch_shapes=[
            *[pltpu.VMEM((p.shape[1] // LANES, p.shape[0], LANES), p.dtype) for p, *_ in parts],
            *[pltpu.VMEM((p.shape[1] // LANES, LANES, p.shape[0]), p.dtype) for p, *_ in parts],
            pltpu.SemaphoreType.DMA((count, max(steps))),
            pltpu.SemaphoreType.DMA((count, max(steps))),
        ],
        input_output_aliases={} if fresh else {count: 0, count + 1: 1},
        compiler_params=pltpu.CompilerParams(vmem_limit_bytes=32 * 2**20),
        cost_estimate=pl.CostEstimate(flops=0, bytes_accessed=moved, transcendentals=0),
    )(*operands)


def doubled(x, axis, pairs, high):
    other = lax.ppermute(x, axis, pairs)
    return jnp.where(high, jnp.concatenate([other, x]), jnp.concatenate([x, other]))


def gathered_gain(gain):
    length = gain.shape[0]
    y, xl, cols = (lax.axis_index(axis) for axis in ("y", "xl", "cols"))
    index = jnp.arange(4)[:, None]
    x = jnp.broadcast_to(gain[None], (4, length))
    for shift in (1, 2, 3):
        part = lax.ppermute(gain, "y", [(i, (i + shift) % 4) for i in range(4)])
        x = jnp.where(index == (y - shift) % 4, part[None], x)
    x = doubled(x, "xl", SWAP, xl == 1)
    for bit in (1, 4, 8):
        pairs = [(i, i ^ bit) for i in range(16)]
        x = doubled(x, "cols", pairs, (cols & bit) != 0)
    pairs = [(i, i ^ 18) for i in range(32)]
    x = doubled(x, ("xl", "cols"), pairs, (cols & 2) != 0)
    x = x.reshape(2, 2, 2, 2, 2, 4, length)
    return x.transpose(5, 4, 1, 2, 0, 3, 6).reshape(-1)


def per_device(train_gate, low_gate, high_gate, train_up, low_up, high_up, norm_train, norm_step):
    rows, width = train_gate.shape
    cut = width * 5 // 7 // LANES * LANES

    def up(v):
        return lax.ppermute(v, "y", UP)

    def down(v):
        return lax.ppermute(v, "y", DOWN)

    def across(v):
        return lax.ppermute(v, "xl", SWAP)

    g = merged(train_gate, low_gate, high_gate)
    u = merged(train_up, low_up, high_up)
    gain = (norm_train + norm_step).astype(jnp.bfloat16)

    g_m, g_x, u_p = up(g), across(g), down(u)
    u_m, u_x, g_p = up(u), across(u), down(g)
    g_f, cg_p, cu_p = up(g_m), down(g_x), across(u_p)
    cu_m0, cu_m1 = across(u_m[:, :cut]), across(u_m[:, cut:])
    cg_m, u_f = up(g_x), down(u_p)
    cg_f0 = across(g_f[:, :cut])
    cg_f1, cu_f1 = down(cg_p[:, cut:]), down(cu_p[:, cut:])
    cu_f0 = up(cu_m0)

    out = jax.ShapeDtypeStruct((width, rows * 8), jnp.bfloat16)
    outs = place((out, out), [(g, 0, 0, 0, 0), (u, 1, 0, 0, 0)])
    outs = place(outs, [(g_m, 0, 0, 3, 0), (g_x, 0, 0, 0, 1), (u_p, 1, 0, 1, 0)])
    outs = place(outs, [(u_m, 1, 0, 3, 0), (u_x, 1, 0, 0, 1), (g_p, 0, 0, 1, 0)])
    outs = place(outs, [(g_f, 0, 0, 2, 0), (cg_p, 0, 0, 1, 1), (cu_p, 1, 0, 1, 1)])
    outs = place(
        outs, [(cu_m0, 1, 0, 3, 1), (cu_m1, 1, cut, 3, 1), (cg_m, 0, 0, 3, 1), (u_f, 1, 0, 2, 0)]
    )
    outs = place(
        outs,
        [(cg_f0, 0, 0, 2, 1), (cg_f1, 0, cut, 2, 1), (cu_f0, 1, 0, 2, 1), (cu_f1, 1, cut, 2, 1)],
    )
    return (*outs, gathered_gain(gain))


def solution(mesh):
    finer = Mesh(mesh.devices.reshape(4, 2, mesh.shape["cols"]), ("y", "xl", "cols"))
    shard, every = ("y", "xl"), ("y", "xl", "cols")
    return jax.shard_map(
        per_device,
        mesh=finer,
        in_specs=(
            P(shard, "cols"),
            P(shard, None),
            P(None, "cols"),
            P(shard, "cols"),
            P(shard, None),
            P(None, "cols"),
            P(every),
            P(every),
        ),
        out_specs=(P("cols", None), P("cols", None), P()),
        check_vma=False,
    )
```

```python
import jax
import jax.numpy as jnp
from jax import lax
from jax.experimental import pallas as pl
from jax.experimental.pallas import tpu as pltpu
from jax.sharding import Mesh
from jax.sharding import PartitionSpec as P


mix_rate = 1.0
LANES = 128
UP = [(i, (i + 1) % 4) for i in range(4)]
DOWN = [(i, (i - 1) % 4) for i in range(4)]
SWAP = [(0, 1), (1, 0)]


def merged(train, low, high):
    change = lax.dot_general(
        low, high, (((0,), (0,)), ((), ())), preferred_element_type=jnp.float32
    )
    return (train.astype(jnp.float32) + mix_rate * change).astype(jnp.bfloat16)


def place(outs, parts, held=False):
    fresh = not isinstance(outs[0], jax.Array)
    count = len(parts)
    steps = [p.shape[1] // LANES for p, *_ in parts]

    def kernel(*refs):
        y, xl = lax.axis_index("y"), lax.axis_index("xl")
        piece_refs, refs = refs[:count], refs[count:]
        refs = refs[0 if fresh else 2 :]
        out_refs, refs = refs[:2], refs[2:]
        taken, refs = ([], refs) if held else (refs[:count], refs[count:])
        turned, (in_sem, out_sem) = refs[:count], refs[count:]

        def load(k, c):
            columns = pl.ds(pl.multiple_of(c * LANES, LANES), LANES)
            return pltpu.make_async_copy(
                piece_refs[k].at[:, columns], taken[k].at[c], in_sem.at[k, c]
            )

        def save(k, c):
            rows = pl.ds(pl.multiple_of(parts[k][2] + c * LANES, LANES), LANES)
            size = parts[k][0].shape[0]
            source = lax.rem(y + parts[k][3], 4) * 2 + lax.rem(xl + parts[k][4], 2)
            columns = pl.ds(pl.multiple_of(source * size, LANES), size)
            return pltpu.make_async_copy(
                turned[k].at[c], out_refs[parts[k][1]].at[rows, columns], out_sem.at[k, c]
            )

        for k in range(count):
            for c in range(0 if held else steps[k]):
                load(k, c).start()
        for k in range(count):

            def step(c):
                if held:
                    turned[k][c] = piece_refs[k][:, c * LANES : (c + 1) * LANES].T
                else:
                    load(k, c).wait()
                    turned[k][c] = taken[k][c].T
                save(k, c).start()

            if held:
                for c in range(steps[k]):
                    step(c)
            else:
                pl.loop(0, steps[k])(step)

        for k in range(count):
            for c in range(steps[k]):
                save(k, c).wait()

    shapes = [jax.ShapeDtypeStruct(o.shape, o.dtype) for o in outs]
    any_spec = pl.BlockSpec(memory_space=pl.ANY)
    operands = [*[p for p, *_ in parts], *([] if fresh else outs)]
    moved = sum(p.size * 2 * 2 for p, *_ in parts)
    return pl.pallas_call(
        kernel,
        out_shape=shapes,
        in_specs=[pl.BlockSpec(memory_space=pltpu.VMEM) if held else any_spec] * count
            + [any_spec] * (len(operands) - count),
        out_specs=[any_spec] * 2,
        scratch_shapes=[
            *([] if held else [pltpu.VMEM((p.shape[1] // LANES, p.shape[0], LANES), p.dtype) for p, *_ in parts]),
            *[pltpu.VMEM((p.shape[1] // LANES, LANES, p.shape[0]), p.dtype) for p, *_ in parts],
            pltpu.SemaphoreType.DMA((count, max(steps))),
            pltpu.SemaphoreType.DMA((count, max(steps))),
        ],
        input_output_aliases={} if fresh else {count: 0, count + 1: 1},
        compiler_params=pltpu.CompilerParams(vmem_limit_bytes=32 * 2**20),
        cost_estimate=pl.CostEstimate(flops=0, bytes_accessed=moved, transcendentals=0),
    )(*operands)


def doubled(x, axis, pairs, high):
    other = lax.ppermute(x, axis, pairs)
    return jnp.where(high, jnp.concatenate([other, x]), jnp.concatenate([x, other]))


def gathered_gain(gain):
    length = gain.shape[0]
    y, xl, cols = (lax.axis_index(axis) for axis in ("y", "xl", "cols"))
    index = jnp.arange(4)[:, None]
    x = jnp.broadcast_to(gain[None], (4, length))
    for shift in (1, 2, 3):
        part = lax.ppermute(gain, "y", [(i, (i + shift) % 4) for i in range(4)])
        x = jnp.where(index == (y - shift) % 4, part[None], x)
    x = doubled(x, "xl", SWAP, xl == 1)
    for bit in (1, 4, 8):
        pairs = [(i, i ^ bit) for i in range(16)]
        x = doubled(x, "cols", pairs, (cols & bit) != 0)
    pairs = [(i, i ^ 18) for i in range(32)]
    x = doubled(x, ("xl", "cols"), pairs, (cols & 2) != 0)
    x = x.reshape(2, 2, 2, 2, 2, 4, length)
    return x.transpose(5, 4, 1, 2, 0, 3, 6).reshape(-1)


def per_device(train_gate, low_gate, high_gate, train_up, low_up, high_up, norm_train, norm_step):
    rows, width = train_gate.shape
    cut = width * 5 // 7 // LANES * LANES

    def up(v):
        return lax.ppermute(v, "y", UP)

    def down(v):
        return lax.ppermute(v, "y", DOWN)

    def across(v):
        return lax.ppermute(v, "xl", SWAP)

    low_g, low_u = low_gate.T, low_up.T
    raw_g_x, raw_g_m, raw_u_p = across(train_gate), up(train_gate), down(train_up)
    low_g_x, low_g_m, low_u_p = across(low_g), up(low_g), down(low_u)
    g = merged(train_gate, low_g, high_gate)
    u = merged(train_up, low_u, high_up)
    gain = (norm_train + norm_step).astype(jnp.bfloat16)

    g_m = merged(raw_g_m, low_g_m, high_gate)
    g_x = merged(raw_g_x, low_g_x, high_gate)
    u_p = merged(raw_u_p, low_u_p, high_up)
    u_m, u_x, g_p = up(u), across(u), down(g)
    g_f, cg_p, cu_p = up(g_m), down(g_x), across(u_p)
    cu_m0, cu_m1 = across(u_m[:, :cut]), across(u_m[:, cut:])
    cg_m, u_f = up(g_x), down(u_p)
    cg_f0 = across(g_f[:, :cut])
    cg_f1, cu_f1 = down(cg_p[:, cut:]), down(cu_p[:, cut:])
    cu_f0 = up(cu_m0)

    out = jax.ShapeDtypeStruct((width, rows * 8), jnp.bfloat16)
    outs = place((out, out), [(g, 0, 0, 0, 0), (u, 1, 0, 0, 0)])
    outs = place(outs, [(g_m, 0, 0, 3, 0), (g_x, 0, 0, 0, 1), (u_p, 1, 0, 1, 0)])
    outs = place(outs, [(u_m, 1, 0, 3, 0), (u_x, 1, 0, 0, 1), (g_p, 0, 0, 1, 0)])
    outs = place(outs, [(g_f, 0, 0, 2, 0), (cg_p, 0, 0, 1, 1), (cu_p, 1, 0, 1, 1)])
    outs = place(
        outs, [(cu_m0, 1, 0, 3, 1), (cu_m1, 1, cut, 3, 1), (cg_m, 0, 0, 3, 1), (u_f, 1, 0, 2, 0)]
    )
    outs = place(
        outs,
        [(cg_f0, 0, 0, 2, 1), (cg_f1, 0, cut, 2, 1), (cu_f0, 1, 0, 2, 1), (cu_f1, 1, cut, 2, 1)],
        held=True,
    )
    return (*outs, gathered_gain(gain))


def solution(mesh):
    finer = Mesh(mesh.devices.reshape(4, 2, mesh.shape["cols"]), ("y", "xl", "cols"))
    shard, every = ("y", "xl"), ("y", "xl", "cols")
    return jax.shard_map(
        per_device,
        mesh=finer,
        in_specs=(
            P(shard, "cols"),
            P(shard, None),
            P(None, "cols"),
            P(shard, "cols"),
            P(shard, None),
            P(None, "cols"),
            P(every),
            P(every),
        ),
        out_specs=(P("cols", None), P("cols", None), P()),
        check_vma=False,
    )
```

```python
import jax
import jax.numpy as jnp
from jax import lax
from jax.experimental import pallas as pl
from jax.experimental.pallas import tpu as pltpu
from jax.sharding import Mesh
from jax.sharding import PartitionSpec as P


mix_rate = 1.0
LANES = 128
SHARE = 512
UP = [(i, (i + 1) % 4) for i in range(4)]
DOWN = [(i, (i - 1) % 4) for i in range(4)]
SWAP = [(0, 1), (1, 0)]


def merged(train, low, high):
    change = lax.dot_general(
        low, high, (((0,), (0,)), ((), ())), preferred_element_type=jnp.float32
    )
    return (train.astype(jnp.float32) + mix_rate * change).astype(jnp.bfloat16)


def place(outs, parts, held=False):
    fresh = not isinstance(outs[0], jax.Array)
    count = len(parts)
    steps = [p.shape[1] // LANES for p, *_ in parts]
    parts = [part if len(part) == 6 else (*part, 0) for part in parts]

    def kernel(*refs):
        y, xl = lax.axis_index("y"), lax.axis_index("xl")
        piece_refs, refs = refs[:count], refs[count:]
        refs = refs[0 if fresh else 2 :]
        out_refs, refs = refs[:2], refs[2:]
        taken, refs = ([], refs) if held else (refs[:count], refs[count:])
        turned, (in_sem, out_sem) = refs[:count], refs[count:]

        def load(k, c):
            columns = pl.ds(pl.multiple_of(c * LANES, LANES), LANES)
            return pltpu.make_async_copy(
                piece_refs[k].at[:, columns], taken[k].at[c], in_sem.at[k, c]
            )

        def save(k, c):
            rows = pl.ds(pl.multiple_of(parts[k][2] + c * LANES, LANES), LANES)
            size = parts[k][0].shape[0]
            source = lax.rem(y + parts[k][3], 4) * 2 + lax.rem(xl + parts[k][4], 2)
            columns = pl.ds(pl.multiple_of(source * SHARE + parts[k][5], LANES), size)
            return pltpu.make_async_copy(
                turned[k].at[c], out_refs[parts[k][1]].at[rows, columns], out_sem.at[k, c]
            )

        for k in range(count):
            for c in range(0 if held else steps[k]):
                load(k, c).start()
        for k in range(count):

            def step(c):
                if held:
                    turned[k][c] = piece_refs[k][:, c * LANES : (c + 1) * LANES].T
                else:
                    load(k, c).wait()
                    turned[k][c] = taken[k][c].T
                save(k, c).start()

            if held:
                for c in range(steps[k]):
                    step(c)
            else:
                pl.loop(0, steps[k])(step)

        for k in range(count):
            for c in range(steps[k]):
                save(k, c).wait()

    shapes = [jax.ShapeDtypeStruct(o.shape, o.dtype) for o in outs]
    any_spec = pl.BlockSpec(memory_space=pl.ANY)
    operands = [*[p for p, *_ in parts], *([] if fresh else outs)]
    moved = sum(p.size * 2 * 2 for p, *_ in parts)
    return pl.pallas_call(
        kernel,
        out_shape=shapes,
        in_specs=[pl.BlockSpec(memory_space=pltpu.VMEM) if held else any_spec] * count
            + [any_spec] * (len(operands) - count),
        out_specs=[any_spec] * 2,
        scratch_shapes=[
            *([] if held else [pltpu.VMEM((p.shape[1] // LANES, p.shape[0], LANES), p.dtype) for p, *_ in parts]),
            *[pltpu.VMEM((p.shape[1] // LANES, LANES, p.shape[0]), p.dtype) for p, *_ in parts],
            pltpu.SemaphoreType.DMA((count, max(steps))),
            pltpu.SemaphoreType.DMA((count, max(steps))),
        ],
        input_output_aliases={} if fresh else {count: 0, count + 1: 1},
        compiler_params=pltpu.CompilerParams(vmem_limit_bytes=32 * 2**20),
        cost_estimate=pl.CostEstimate(flops=0, bytes_accessed=moved, transcendentals=0),
    )(*operands)


def doubled(x, axis, pairs, high):
    other = lax.ppermute(x, axis, pairs)
    return jnp.where(high, jnp.concatenate([other, x]), jnp.concatenate([x, other]))


def gathered_gain(gain):
    length = gain.shape[0]
    y, xl, cols = (lax.axis_index(axis) for axis in ("y", "xl", "cols"))
    index = jnp.arange(4)[:, None]
    x = jnp.broadcast_to(gain[None], (4, length))
    for shift in (1, 2, 3):
        part = lax.ppermute(gain, "y", [(i, (i + shift) % 4) for i in range(4)])
        x = jnp.where(index == (y - shift) % 4, part[None], x)
    x = doubled(x, "xl", SWAP, xl == 1)
    for bit in (1, 4, 8):
        pairs = [(i, i ^ bit) for i in range(16)]
        x = doubled(x, "cols", pairs, (cols & bit) != 0)
    pairs = [(i, i ^ 18) for i in range(32)]
    x = doubled(x, ("xl", "cols"), pairs, (cols & 2) != 0)
    x = x.reshape(2, 2, 2, 2, 2, 4, length)
    return x.transpose(5, 4, 1, 2, 0, 3, 6).reshape(-1)


def per_device(train_gate, low_gate, high_gate, train_up, low_up, high_up, norm_train, norm_step):
    rows, width = train_gate.shape

    def up(v):
        return lax.ppermute(v, "y", UP)

    def down(v):
        return lax.ppermute(v, "y", DOWN)

    def across(v):
        return lax.ppermute(v, "xl", SWAP)

    low_g, low_u = low_gate.T, low_up.T
    raw_g_x, raw_g_m, raw_u_p = across(train_gate), up(train_gate), down(train_up)
    low_g_x, low_g_m, low_u_p = across(low_g), up(low_g), down(low_u)
    g = merged(train_gate, low_g, high_gate)
    u = merged(train_up, low_u, high_up)
    gain = (norm_train + norm_step).astype(jnp.bfloat16)

    g_m = merged(raw_g_m, low_g_m, high_gate)
    g_x = merged(raw_g_x, low_g_x, high_gate)
    u_p = merged(raw_u_p, low_u_p, high_up)
    u_m, u_x, g_p = up(u), across(u), down(g)
    g_f, cg_p, cu_p = up(g_m), down(g_x), across(u_p)
    near, mid, late = width * 4 // 7, width * 5 // 7, width * 6 // 7
    cu_m0, cu_m1, cu_m2 = (across(u_m[:, :near]), across(u_m[:, near:mid]), across(u_m[:, mid:]))
    cg_m, u_f = up(g_x), down(u_p)
    cg_f0, cg_f1 = across(g_f[:, :near]), across(g_f[LANES:, near:mid])
    cg_f2, cg_f3 = down(cg_p[:, mid:]), down(cg_p[:LANES, near:mid])
    cu_f2, cu_f3 = down(cu_p[:, mid:late]), down(cu_p[:, late:])
    cu_f0, cu_f1 = up(cu_m0), up(cu_m1)

    out = jax.ShapeDtypeStruct((width, rows * 8), jnp.bfloat16)
    outs = place((out, out), [(g, 0, 0, 0, 0), (u, 1, 0, 0, 0)])
    outs = place(outs, [(g_m, 0, 0, 3, 0), (g_x, 0, 0, 0, 1), (u_p, 1, 0, 1, 0)])
    outs = place(outs, [(u_m, 1, 0, 3, 0), (u_x, 1, 0, 0, 1), (g_p, 0, 0, 1, 0)])
    outs = place(outs, [(g_f, 0, 0, 2, 0), (cg_p, 0, 0, 1, 1), (cu_p, 1, 0, 1, 1)])
    outs = place(
        outs,
        [
            (cu_m0, 1, 0, 3, 1),
            (cu_m1, 1, near, 3, 1),
            (cu_m2, 1, mid, 3, 1),
            (cg_m, 0, 0, 3, 1),
            (u_f, 1, 0, 2, 0),
        ],
    )
    outs = place(
        outs,
        [
            (cg_f0, 0, 0, 2, 1),
            (cu_f0, 1, 0, 2, 1),
            (cg_f2, 0, mid, 2, 1),
            (cg_f3, 0, near, 2, 1),
            (cu_f2, 1, mid, 2, 1),
        ],
        held=True,
    )
    outs = place(
        outs,
        [(cg_f1, 0, near, 2, 1, LANES), (cu_f1, 1, near, 2, 1), (cu_f3, 1, late, 2, 1)],
        held=True,
    )
    return (*outs, gathered_gain(gain))


def solution(mesh):
    finer = Mesh(mesh.devices.reshape(4, 2, mesh.shape["cols"]), ("y", "xl", "cols"))
    shard, every = ("y", "xl"), ("y", "xl", "cols")
    return jax.shard_map(
        per_device,
        mesh=finer,
        in_specs=(
            P(shard, "cols"),
            P(shard, None),
            P(None, "cols"),
            P(shard, "cols"),
            P(shard, None),
            P(None, "cols"),
            P(every),
            P(every),
        ),
        out_specs=(P("cols", None), P("cols", None), P()),
        check_vma=False,
    )
```

```python
import jax
import jax.numpy as jnp
from jax import lax
from jax.experimental import pallas as pl
from jax.experimental.pallas import tpu as pltpu
from jax.sharding import Mesh
from jax.sharding import PartitionSpec as P


mix_rate = 1.0
LANES = 128
SHARE = 512
UP = [(i, (i + 1) % 4) for i in range(4)]
DOWN = [(i, (i - 1) % 4) for i in range(4)]
SWAP = [(0, 1), (1, 0)]


def merged(train, low, high):
    change = lax.dot_general(
        low, high, (((0,), (0,)), ((), ())), preferred_element_type=jnp.float32
    )
    return (train.astype(jnp.float32) + mix_rate * change).astype(jnp.bfloat16)


def place(outs, parts, held=False):
    fresh = not isinstance(outs[0], jax.Array)
    count = len(parts)
    steps = [p.shape[1] // LANES for p, *_ in parts]
    parts = [part if len(part) == 6 else (*part, 0) for part in parts]

    def kernel(*refs):
        y, xl = lax.axis_index("y"), lax.axis_index("xl")
        piece_refs, refs = refs[:count], refs[count:]
        refs = refs[0 if fresh else 2 :]
        out_refs, refs = refs[:2], refs[2:]
        taken, refs = ([], refs) if held else (refs[:count], refs[count:])
        turned, (in_sem, out_sem) = refs[:count], refs[count:]

        def load(k, c):
            columns = pl.ds(pl.multiple_of(c * LANES, LANES), LANES)
            return pltpu.make_async_copy(
                piece_refs[k].at[:, columns], taken[k].at[c], in_sem.at[k, c]
            )

        def save(k, c):
            rows = pl.ds(pl.multiple_of(parts[k][2] + c * LANES, LANES), LANES)
            size = parts[k][0].shape[0]
            source = lax.rem(y + parts[k][3], 4) * 2 + lax.rem(xl + parts[k][4], 2)
            columns = pl.ds(pl.multiple_of(source * SHARE + parts[k][5], LANES), size)
            return pltpu.make_async_copy(
                turned[k].at[c], out_refs[parts[k][1]].at[rows, columns], out_sem.at[k, c]
            )

        for k in range(count):
            for c in range(0 if held else steps[k]):
                load(k, c).start()
        for k in range(count):

            def step(c):
                if held:
                    turned[k][c] = piece_refs[k][:, c * LANES : (c + 1) * LANES].T
                else:
                    load(k, c).wait()
                    turned[k][c] = taken[k][c].T
                save(k, c).start()

            if held:
                for c in range(steps[k]):
                    step(c)
            else:
                pl.loop(0, steps[k])(step)

        for k in range(count):
            for c in range(steps[k]):
                save(k, c).wait()

    shapes = [jax.ShapeDtypeStruct(o.shape, o.dtype) for o in outs]
    any_spec = pl.BlockSpec(memory_space=pl.ANY)
    operands = [*[p for p, *_ in parts], *([] if fresh else outs)]
    moved = sum(p.size * 2 * 2 for p, *_ in parts)
    return pl.pallas_call(
        kernel,
        out_shape=shapes,
        in_specs=[pl.BlockSpec(memory_space=pltpu.VMEM) if held else any_spec] * count
            + [any_spec] * (len(operands) - count),
        out_specs=[any_spec] * 2,
        scratch_shapes=[
            *([] if held else [pltpu.VMEM((p.shape[1] // LANES, p.shape[0], LANES), p.dtype) for p, *_ in parts]),
            *[pltpu.VMEM((p.shape[1] // LANES, LANES, p.shape[0]), p.dtype) for p, *_ in parts],
            pltpu.SemaphoreType.DMA((count, max(steps))),
            pltpu.SemaphoreType.DMA((count, max(steps))),
        ],
        input_output_aliases={} if fresh else {count: 0, count + 1: 1},
        compiler_params=pltpu.CompilerParams(vmem_limit_bytes=32 * 2**20),
        cost_estimate=pl.CostEstimate(flops=0, bytes_accessed=moved, transcendentals=0),
    )(*operands)


def doubled(x, axis, pairs, high):
    other = lax.ppermute(x, axis, pairs)
    return jnp.where(high, jnp.concatenate([other, x]), jnp.concatenate([x, other]))


def gathered_gain(gain):
    length = gain.shape[0]
    y, xl, cols = (lax.axis_index(axis) for axis in ("y", "xl", "cols"))
    index = jnp.arange(4)[:, None]
    x = jnp.broadcast_to(gain[None], (4, length))
    for shift in (1, 2, 3):
        part = lax.ppermute(gain, "y", [(i, (i + shift) % 4) for i in range(4)])
        x = jnp.where(index == (y - shift) % 4, part[None], x)
    x = doubled(x, "xl", SWAP, xl == 1)
    for bit in (1, 4, 8):
        pairs = [(i, i ^ bit) for i in range(16)]
        x = doubled(x, "cols", pairs, (cols & bit) != 0)
    pairs = [(i, i ^ 18) for i in range(32)]
    x = doubled(x, ("xl", "cols"), pairs, (cols & 2) != 0)
    x = x.reshape(2, 2, 2, 2, 2, 4, length)
    return x.transpose(5, 4, 1, 2, 0, 3, 6).reshape(-1)


def per_device(train_gate, low_gate, high_gate, train_up, low_up, high_up, norm_train, norm_step):
    rows, width = train_gate.shape

    def up(v):
        return lax.ppermute(v, "y", UP)

    def down(v):
        return lax.ppermute(v, "y", DOWN)

    def across(v):
        return lax.ppermute(v, "xl", SWAP)

    low_g, low_u = low_gate.T, low_up.T
    raw_g_x, raw_g_m, raw_u_p = across(train_gate), up(train_gate), down(train_up)
    low_g_x, low_g_m, low_u_p = across(low_g), up(low_g), down(low_u)
    g = merged(train_gate, low_g, high_gate)
    u = merged(train_up, low_u, high_up)
    gain = (norm_train + norm_step).astype(jnp.bfloat16)

    g_m = merged(raw_g_m, low_g_m, high_gate)
    g_x = merged(raw_g_x, low_g_x, high_gate)
    u_p = merged(raw_u_p, low_u_p, high_up)
    u_m, u_x, g_p = up(u), across(u), down(g)
    g_f, cg_p, cu_p = up(g_m), down(g_x), across(u_p)
    first, near, mid, late = width * 2 // 7, width * 4 // 7, width * 5 // 7, width * 6 // 7
    cu_m0, cu_m1, cu_m2 = (across(u_m[:, :near]), across(u_m[:, near:mid]), across(u_m[:, mid:]))
    cg_m, u_f = up(g_x), down(u_p)
    cg_f0, cg_f4, cg_f1 = (across(g_f[:, :first]), across(g_f[:, first:near]), across(g_f[LANES:, near:mid]))
    cg_f2, cg_f3 = down(cg_p[:, mid:]), down(cg_p[:LANES, near:mid])
    cu_f2, cu_f3 = down(cu_p[:, mid:late]), down(cu_p[:, late:])
    cu_f4 = down(cu_p[:LANES, near:mid])
    cu_f0, cu_f1 = up(cu_m0), up(cu_m1[LANES:])

    out = jax.ShapeDtypeStruct((width, rows * 8), jnp.bfloat16)
    outs = place((out, out), [(g, 0, 0, 0, 0), (u, 1, 0, 0, 0)])
    outs = place(outs, [(g_m, 0, 0, 3, 0), (g_x, 0, 0, 0, 1), (u_p, 1, 0, 1, 0)])
    outs = place(outs, [(u_m, 1, 0, 3, 0), (u_x, 1, 0, 0, 1), (g_p, 0, 0, 1, 0)])
    outs = place(outs, [(g_f, 0, 0, 2, 0), (cg_p, 0, 0, 1, 1), (cu_p, 1, 0, 1, 1)])
    outs = place(
        outs,
        [
            (cu_m0, 1, 0, 3, 1),
            (cu_m1, 1, near, 3, 1),
            (cu_m2, 1, mid, 3, 1),
            (cg_m, 0, 0, 3, 1),
            (u_f, 1, 0, 2, 0),
        ],
    )
    outs = place(outs, [(cg_f2, 0, mid, 2, 1), (cg_f3, 0, near, 2, 1), (cu_f4, 1, near, 2, 1), (cg_f0, 0, 0, 2, 1)], held=True)
    outs = place(outs, [(cg_f4, 0, first, 2, 1), (cu_f0, 1, 0, 2, 1), (cu_f2, 1, mid, 2, 1)], held=True)
    outs = place(
        outs, [(cg_f1, 0, near, 2, 1, LANES), (cu_f1, 1, near, 2, 1, LANES), (cu_f3, 1, late, 2, 1)], held=True
    )
    return (*outs, gathered_gain(gain))


def solution(mesh):
    finer = Mesh(mesh.devices.reshape(4, 2, mesh.shape["cols"]), ("y", "xl", "cols"))
    shard, every = ("y", "xl"), ("y", "xl", "cols")
    return jax.shard_map(
        per_device,
        mesh=finer,
        in_specs=(
            P(shard, "cols"),
            P(shard, None),
            P(None, "cols"),
            P(shard, "cols"),
            P(shard, None),
            P(None, "cols"),
            P(every),
            P(every),
        ),
        out_specs=(P("cols", None), P("cols", None), P()),
        check_vma=False,
    )
```

```python
import jax
import jax.numpy as jnp
from jax import lax
from jax.experimental import pallas as pl
from jax.experimental.pallas import tpu as pltpu
from jax.sharding import Mesh
from jax.sharding import PartitionSpec as P


mix_rate = 1.0
LANES = 128
SHARE = 512
UP = [(i, (i + 1) % 4) for i in range(4)]
DOWN = [(i, (i - 1) % 4) for i in range(4)]
SWAP = [(0, 1), (1, 0)]


def merged(train, low, high):
    change = lax.dot_general(
        low, high, (((0,), (0,)), ((), ())), preferred_element_type=jnp.float32
    )
    return (train.astype(jnp.float32) + mix_rate * change).astype(jnp.bfloat16)


def place(outs, parts, held=False):
    fresh = not isinstance(outs[0], jax.Array)
    count = len(parts)
    steps = [p.shape[1] // LANES for p, *_ in parts]
    parts = [part if len(part) == 6 else (*part, 0) for part in parts]

    def kernel(*refs):
        y, xl = lax.axis_index("y"), lax.axis_index("xl")
        piece_refs, refs = refs[:count], refs[count:]
        refs = refs[0 if fresh else 2 :]
        out_refs, refs = refs[:2], refs[2:]
        taken, refs = ([], refs) if held else (refs[:count], refs[count:])
        turned, (in_sem, out_sem) = refs[:count], refs[count:]

        def load(k, c):
            columns = pl.ds(pl.multiple_of(c * LANES, LANES), LANES)
            return pltpu.make_async_copy(
                piece_refs[k].at[:, columns], taken[k].at[c], in_sem.at[k, c]
            )

        def save(k, c):
            rows = pl.ds(pl.multiple_of(parts[k][2] + c * LANES, LANES), LANES)
            size = parts[k][0].shape[0]
            source = lax.rem(y + parts[k][3], 4) * 2 + lax.rem(xl + parts[k][4], 2)
            columns = pl.ds(pl.multiple_of(source * SHARE + parts[k][5], LANES), size)
            return pltpu.make_async_copy(
                turned[k].at[c], out_refs[parts[k][1]].at[rows, columns], out_sem.at[k, c]
            )

        for k in range(count):
            for c in range(0 if held else steps[k]):
                load(k, c).start()
        for k in range(count):

            def step(c):
                if held:
                    turned[k][c] = piece_refs[k][:, c * LANES : (c + 1) * LANES].T
                else:
                    load(k, c).wait()
                    turned[k][c] = taken[k][c].T
                save(k, c).start()

            if held:
                for c in range(steps[k]):
                    step(c)
            else:
                pl.loop(0, steps[k])(step)

        for k in range(count):
            for c in range(steps[k]):
                save(k, c).wait()

    shapes = [jax.ShapeDtypeStruct(o.shape, o.dtype) for o in outs]
    any_spec = pl.BlockSpec(memory_space=pl.ANY)
    operands = [*[p for p, *_ in parts], *([] if fresh else outs)]
    moved = sum(p.size * 2 * 2 for p, *_ in parts)
    return pl.pallas_call(
        kernel,
        out_shape=shapes,
        in_specs=[pl.BlockSpec(memory_space=pltpu.VMEM) if held else any_spec] * count
            + [any_spec] * (len(operands) - count),
        out_specs=[any_spec] * 2,
        scratch_shapes=[
            *([] if held else [pltpu.VMEM((p.shape[1] // LANES, p.shape[0], LANES), p.dtype) for p, *_ in parts]),
            *[pltpu.VMEM((p.shape[1] // LANES, LANES, p.shape[0]), p.dtype) for p, *_ in parts],
            pltpu.SemaphoreType.DMA((count, max(steps))),
            pltpu.SemaphoreType.DMA((count, max(steps))),
        ],
        input_output_aliases={} if fresh else {count: 0, count + 1: 1},
        compiler_params=pltpu.CompilerParams(vmem_limit_bytes=32 * 2**20),
        cost_estimate=pl.CostEstimate(flops=0, bytes_accessed=moved, transcendentals=0),
    )(*operands)


def doubled(x, axis, pairs, high):
    other = lax.ppermute(x, axis, pairs)
    return jnp.where(high, jnp.concatenate([other, x]), jnp.concatenate([x, other]))


def gathered_gain(gain):
    length = gain.shape[0]
    y, xl, cols = (lax.axis_index(axis) for axis in ("y", "xl", "cols"))
    x_hi = (cols >> 1) & 1
    x = gain[None]
    for bit in (1, 4, 8):
        pairs = [(i, i ^ bit) for i in range(16)]
        x = doubled(x, "cols", pairs, (cols & bit) != 0)
    pairs = [(i, i ^ 18) for i in range(32)]
    x = doubled(x, ("xl", "cols"), pairs, x_hi == 1)
    index = jnp.arange(4)[:, None, None]
    mine = jnp.broadcast_to(x[None], (4, *x.shape))
    for shift in (1, 2, 3):
        part = lax.ppermute(x, "y", [(i, (i + shift) % 4) for i in range(4)])
        mine = jnp.where(index == (y - shift) % 4, part[None], mine)
    other = lax.ppermute(mine, "xl", SWAP)
    mine, other = (v.reshape(4, 1, 2, 2, 2, 2, length) for v in (mine, other))
    both = jnp.arange(2)
    own = (both[:, None] ^ both[None, :] ^ xl ^ x_hi) == 0
    x = jnp.where(own.reshape(1, 2, 2, 1, 1, 1, 1), mine, other)
    return x.transpose(0, 1, 3, 4, 2, 5, 6).reshape(-1)


def per_device(train_gate, low_gate, high_gate, train_up, low_up, high_up, norm_train, norm_step):
    rows, width = train_gate.shape

    def up(v):
        return lax.ppermute(v, "y", UP)

    def down(v):
        return lax.ppermute(v, "y", DOWN)

    def across(v):
        return lax.ppermute(v, "xl", SWAP)

    low_g, low_u = low_gate.T, low_up.T
    raw_g_x, raw_g_m, raw_u_p = across(train_gate), up(train_gate), down(train_up)
    low_g_x, low_g_m, low_u_p = across(low_g), up(low_g), down(low_u)
    g = merged(train_gate, low_g, high_gate)
    u = merged(train_up, low_u, high_up)
    gain = (norm_train + norm_step).astype(jnp.bfloat16)

    g_m = merged(raw_g_m, low_g_m, high_gate)
    g_x = merged(raw_g_x, low_g_x, high_gate)
    u_p = merged(raw_u_p, low_u_p, high_up)
    u_m, u_x, g_p = up(u), across(u), down(g)
    g_f, cg_p, cu_p = up(g_m), down(g_x), across(u_p)
    first, near, mid, late = width * 2 // 7, width * 4 // 7, width * 5 // 7, width * 6 // 7
    cu_m0, cu_m1, cu_m2 = (across(u_m[:, :near]), across(u_m[:, near:mid]), across(u_m[:, mid:]))
    cg_m, u_f = up(g_x), down(u_p)
    cg_f0, cg_f4, cg_f1 = (across(g_f[:, :first]), across(g_f[:, first:near]), across(g_f[LANES:, near:mid]))
    cg_f2, cg_f3 = down(cg_p[:, mid:]), down(cg_p[:LANES, near:mid])
    cu_f2, cu_f3 = down(cu_p[:, mid:late]), down(cu_p[:, late:])
    cu_f0, cu_f1 = up(cu_m0), up(cu_m1)

    out = jax.ShapeDtypeStruct((width, rows * 8), jnp.bfloat16)
    outs = place((out, out), [(g, 0, 0, 0, 0), (u, 1, 0, 0, 0)])
    outs = place(outs, [(g_m, 0, 0, 3, 0), (g_x, 0, 0, 0, 1), (u_p, 1, 0, 1, 0)])
    outs = place(outs, [(u_m, 1, 0, 3, 0), (u_x, 1, 0, 0, 1), (g_p, 0, 0, 1, 0)])
    outs = place(outs, [(g_f, 0, 0, 2, 0), (cg_p, 0, 0, 1, 1), (cu_p, 1, 0, 1, 1)])
    outs = place(
        outs,
        [
            (cu_m0, 1, 0, 3, 1),
            (cu_m1, 1, near, 3, 1),
            (cu_m2, 1, mid, 3, 1),
            (cg_m, 0, 0, 3, 1),
            (u_f, 1, 0, 2, 0),
        ],
    )
    outs = place(outs, [(cg_f2, 0, mid, 2, 1), (cg_f3, 0, near, 2, 1), (cg_f0, 0, 0, 2, 1)], held=True)
    outs = place(outs, [(cg_f4, 0, first, 2, 1), (cu_f0, 1, 0, 2, 1), (cu_f2, 1, mid, 2, 1)], held=True)
    outs = place(outs, [(cg_f1, 0, near, 2, 1, LANES), (cu_f1, 1, near, 2, 1), (cu_f3, 1, late, 2, 1)], held=True)
    return (*outs, gathered_gain(gain))


def solution(mesh):
    finer = Mesh(mesh.devices.reshape(4, 2, mesh.shape["cols"]), ("y", "xl", "cols"))
    shard, every = ("y", "xl"), ("y", "xl", "cols")
    return jax.shard_map(
        per_device,
        mesh=finer,
        in_specs=(
            P(shard, "cols"),
            P(shard, None),
            P(None, "cols"),
            P(shard, "cols"),
            P(shard, None),
            P(None, "cols"),
            P(every),
            P(every),
        ),
        out_specs=(P("cols", None), P("cols", None), P()),
        check_vma=False,
    )
```

```python
import jax
import jax.numpy as jnp
from jax import lax
from jax.experimental import pallas as pl
from jax.experimental.pallas import tpu as pltpu
from jax.sharding import Mesh
from jax.sharding import PartitionSpec as P


mix_rate = 1.0
LANES = 128
SHARE = 512
UP = [(i, (i + 1) % 4) for i in range(4)]
DOWN = [(i, (i - 1) % 4) for i in range(4)]
SWAP = [(0, 1), (1, 0)]


def merged(train, low, high):
    change = lax.dot_general(
        low, high, (((0,), (0,)), ((), ())), preferred_element_type=jnp.float32
    )
    return (train.astype(jnp.float32) + mix_rate * change).astype(jnp.bfloat16)


def place(outs, parts, held=False):
    fresh = not isinstance(outs[0], jax.Array)
    count = len(parts)
    steps = [p.shape[1] // LANES for p, *_ in parts]
    parts = [part if len(part) == 6 else (*part, 0) for part in parts]

    def kernel(*refs):
        y, xl = lax.axis_index("y"), lax.axis_index("xl")
        piece_refs, refs = refs[:count], refs[count:]
        refs = refs[0 if fresh else 2 :]
        out_refs, refs = refs[:2], refs[2:]
        taken, refs = ([], refs) if held else (refs[:count], refs[count:])
        turned, (in_sem, out_sem) = refs[:count], refs[count:]

        def load(k, c):
            columns = pl.ds(pl.multiple_of(c * LANES, LANES), LANES)
            return pltpu.make_async_copy(
                piece_refs[k].at[:, columns], taken[k].at[c], in_sem.at[k, c]
            )

        def save(k, c):
            rows = pl.ds(pl.multiple_of(parts[k][2] + c * LANES, LANES), LANES)
            size = parts[k][0].shape[0]
            source = lax.rem(y + parts[k][3], 4) * 2 + lax.rem(xl + parts[k][4], 2)
            columns = pl.ds(pl.multiple_of(source * SHARE + parts[k][5], LANES), size)
            return pltpu.make_async_copy(
                turned[k].at[c], out_refs[parts[k][1]].at[rows, columns], out_sem.at[k, c]
            )

        for k in range(count):
            for c in range(0 if held else steps[k]):
                load(k, c).start()
        for k in range(count):

            def step(c):
                if held:
                    turned[k][c] = piece_refs[k][:, c * LANES : (c + 1) * LANES].T
                else:
                    load(k, c).wait()
                    turned[k][c] = taken[k][c].T
                save(k, c).start()

            if held:
                for c in range(steps[k]):
                    step(c)
            else:
                pl.loop(0, steps[k])(step)

        for k in range(count):
            for c in range(steps[k]):
                save(k, c).wait()

    shapes = [jax.ShapeDtypeStruct(o.shape, o.dtype) for o in outs]
    any_spec = pl.BlockSpec(memory_space=pl.ANY)
    operands = [*[p for p, *_ in parts], *([] if fresh else outs)]
    moved = sum(p.size * 2 * 2 for p, *_ in parts)
    return pl.pallas_call(
        kernel,
        out_shape=shapes,
        in_specs=[pl.BlockSpec(memory_space=pltpu.VMEM) if held else any_spec] * count
            + [any_spec] * (len(operands) - count),
        out_specs=[any_spec] * 2,
        scratch_shapes=[
            *([] if held else [pltpu.VMEM((p.shape[1] // LANES, p.shape[0], LANES), p.dtype) for p, *_ in parts]),
            *[pltpu.VMEM((p.shape[1] // LANES, LANES, p.shape[0]), p.dtype) for p, *_ in parts],
            pltpu.SemaphoreType.DMA((count, max(steps))),
            pltpu.SemaphoreType.DMA((count, max(steps))),
        ],
        input_output_aliases={} if fresh else {count: 0, count + 1: 1},
        compiler_params=pltpu.CompilerParams(vmem_limit_bytes=32 * 2**20),
        cost_estimate=pl.CostEstimate(flops=0, bytes_accessed=moved, transcendentals=0),
    )(*operands)


def doubled(x, axis, pairs, high):
    other = lax.ppermute(x, axis, pairs)
    return jnp.where(high, jnp.concatenate([other, x]), jnp.concatenate([x, other]))


def gathered_gain(gain):
    length = gain.shape[0]
    y, xl, cols = (lax.axis_index(axis) for axis in ("y", "xl", "cols"))
    x_hi = (cols >> 1) & 1
    x = gain[None]
    for bit in (1, 4, 8):
        pairs = [(i, i ^ bit) for i in range(16)]
        x = doubled(x, "cols", pairs, (cols & bit) != 0)
    pairs = [(i, i ^ 18) for i in range(32)]
    x = doubled(x, ("xl", "cols"), pairs, x_hi == 1)
    index = jnp.arange(4)[:, None, None]
    mine = jnp.broadcast_to(x[None], (4, *x.shape))
    for shift in (1, 2, 3):
        part = lax.ppermute(x, "y", [(i, (i + shift) % 4) for i in range(4)])
        mine = jnp.where(index == (y - shift) % 4, part[None], mine)
    other = lax.ppermute(mine, "xl", SWAP)
    mine, other = (v.reshape(4, 1, 2, 2, 2, 2, length) for v in (mine, other))
    both = jnp.arange(2)
    own = (both[:, None] ^ both[None, :] ^ xl ^ x_hi) == 0
    x = jnp.where(own.reshape(1, 2, 2, 1, 1, 1, 1), mine, other)
    return x.transpose(0, 1, 3, 4, 2, 5, 6).reshape(-1)


def per_device(train_gate, low_gate, high_gate, train_up, low_up, high_up, norm_train, norm_step):
    rows, width = train_gate.shape

    def up(v):
        return lax.ppermute(v, "y", UP)

    def down(v):
        return lax.ppermute(v, "y", DOWN)

    def across(v):
        return lax.ppermute(v, "xl", SWAP)

    low_g, low_u = low_gate.T, low_up.T
    raw_g_x, raw_g_m, raw_u_p = across(train_gate), up(train_gate), down(train_up)
    low_g_x, low_g_m, low_u_p = across(low_g), up(low_g), down(low_u)
    g = merged(train_gate, low_g, high_gate)
    u = merged(train_up, low_u, high_up)
    gain = (norm_train + norm_step).astype(jnp.bfloat16)

    g_m = merged(raw_g_m, low_g_m, high_gate)
    g_x = merged(raw_g_x, low_g_x, high_gate)
    u_p = merged(raw_u_p, low_u_p, high_up)
    u_m, u_x, g_p = up(u), across(u), down(g)
    g_f, cg_p, cu_p = up(g_m), down(g_x), across(u_p)
    first, near, mid, late = width * 2 // 7, width * 4 // 7, width * 5 // 7, width * 6 // 7
    cu_m0, cu_m1, cu_m2 = (across(u_m[:, :near]), across(u_m[:, near:mid]), across(u_m[:, mid:]))
    cg_m, u_f = up(g_x), down(u_p)
    cg_f0, cg_f4, cg_f1 = (across(g_f[:, :first]), across(g_f[:, first:near]), across(g_f[LANES:, near:mid]))
    cg_f2, cg_f3 = down(cg_p[:, mid:]), down(cg_p[:LANES, near:mid])
    cu_f2, cu_f3 = down(cu_p[:, mid:late]), down(cu_p[:, late:])
    cu_f4 = down(cu_p[:LANES, near:mid])
    cu_f0, cu_f1 = up(cu_m0), up(cu_m1[LANES:])

    out = jax.ShapeDtypeStruct((width, rows * 8), jnp.bfloat16)
    outs = place((out, out), [(g, 0, 0, 0, 0), (u, 1, 0, 0, 0)])
    outs = place(outs, [(g_m, 0, 0, 3, 0), (g_x, 0, 0, 0, 1), (u_p, 1, 0, 1, 0)])
    outs = place(outs, [(u_m, 1, 0, 3, 0), (u_x, 1, 0, 0, 1), (g_p, 0, 0, 1, 0)])
    outs = place(outs, [(g_f, 0, 0, 2, 0), (cg_p, 0, 0, 1, 1), (cu_p, 1, 0, 1, 1)])
    outs = place(
        outs,
        [
            (cu_m0, 1, 0, 3, 1),
            (cu_m1, 1, near, 3, 1),
            (cu_m2, 1, mid, 3, 1),
            (cg_m, 0, 0, 3, 1),
            (u_f, 1, 0, 2, 0),
        ],
    )
    outs = place(outs, [(cg_f2, 0, mid, 2, 1), (cg_f3, 0, near, 2, 1), (cu_f4, 1, near, 2, 1), (cg_f0, 0, 0, 2, 1)], held=True)
    outs = place(outs, [(cg_f4, 0, first, 2, 1), (cu_f0, 1, 0, 2, 1), (cu_f2, 1, mid, 2, 1)], held=True)
    outs = place(
        outs, [(cg_f1, 0, near, 2, 1, LANES), (cu_f1, 1, near, 2, 1, LANES), (cu_f3, 1, late, 2, 1)], held=True
    )
    return (*outs, gathered_gain(gain))


def solution(mesh):
    finer = Mesh(mesh.devices.reshape(4, 2, mesh.shape["cols"]), ("y", "xl", "cols"))
    shard, every = ("y", "xl"), ("y", "xl", "cols")
    return jax.shard_map(
        per_device,
        mesh=finer,
        in_specs=(
            P(shard, "cols"),
            P(shard, None),
            P(None, "cols"),
            P(shard, "cols"),
            P(shard, None),
            P(None, "cols"),
            P(every),
            P(every),
        ),
        out_specs=(P("cols", None), P("cols", None), P()),
        check_vma=False,
    )
```

```python
import jax
import jax.numpy as jnp
from jax import lax
from jax.experimental import pallas as pl
from jax.experimental.pallas import tpu as pltpu
from jax.sharding import Mesh
from jax.sharding import PartitionSpec as P


mix_rate = 1.0
LANES = 128
SHARE = 512
UP = [(i, (i + 1) % 4) for i in range(4)]
DOWN = [(i, (i - 1) % 4) for i in range(4)]
SWAP = [(0, 1), (1, 0)]


def merged(train, low, high):
    change = lax.dot_general(
        low, high, (((0,), (0,)), ((), ())), preferred_element_type=jnp.float32
    )
    return (train.astype(jnp.float32) + mix_rate * change).astype(jnp.bfloat16)


def place(outs, parts, held=False):
    fresh = not isinstance(outs[0], jax.Array)
    count = len(parts)
    steps = [p.shape[1] // LANES for p, *_ in parts]
    parts = [part if len(part) == 6 else (*part, 0) for part in parts]

    def kernel(*refs):
        y, xl = lax.axis_index("y"), lax.axis_index("xl")
        piece_refs, refs = refs[:count], refs[count:]
        refs = refs[0 if fresh else 2 :]
        out_refs, refs = refs[:2], refs[2:]
        taken, refs = ([], refs) if held else (refs[:count], refs[count:])
        turned, (in_sem, out_sem) = refs[:count], refs[count:]

        def load(k, c):
            columns = pl.ds(pl.multiple_of(c * LANES, LANES), LANES)
            return pltpu.make_async_copy(
                piece_refs[k].at[:, columns], taken[k].at[c], in_sem.at[k, c]
            )

        def save(k, c):
            rows = pl.ds(pl.multiple_of(parts[k][2] + c * LANES, LANES), LANES)
            size = parts[k][0].shape[0]
            source = lax.rem(y + parts[k][3], 4) * 2 + lax.rem(xl + parts[k][4], 2)
            columns = pl.ds(pl.multiple_of(source * SHARE + parts[k][5], LANES), size)
            return pltpu.make_async_copy(
                turned[k].at[c], out_refs[parts[k][1]].at[rows, columns], out_sem.at[k, c]
            )

        for k in range(0 if held else count):

            @pl.loop(0, steps[k])
            def _(c):
                load(k, c).start()

        for k in range(count):

            def step(c):
                if held:
                    turned[k][c] = piece_refs[k][:, c * LANES : (c + 1) * LANES].T
                else:
                    load(k, c).wait()
                    turned[k][c] = taken[k][c].T
                save(k, c).start()

            if held:
                for c in range(steps[k]):
                    step(c)
            else:
                pl.loop(0, steps[k])(step)

        for k in range(count):
            if held:
                for c in range(steps[k]):
                    save(k, c).wait()
            else:

                @pl.loop(0, steps[k])
                def _(c):
                    save(k, c).wait()


    shapes = [jax.ShapeDtypeStruct(o.shape, o.dtype) for o in outs]
    any_spec = pl.BlockSpec(memory_space=pl.ANY)
    operands = [*[p for p, *_ in parts], *([] if fresh else outs)]
    moved = sum(p.size * 2 * 2 for p, *_ in parts)
    return pl.pallas_call(
        kernel,
        out_shape=shapes,
        in_specs=[pl.BlockSpec(memory_space=pltpu.VMEM) if held else any_spec] * count
            + [any_spec] * (len(operands) - count),
        out_specs=[any_spec] * 2,
        scratch_shapes=[
            *([] if held else [pltpu.VMEM((p.shape[1] // LANES, p.shape[0], LANES), p.dtype) for p, *_ in parts]),
            *[pltpu.VMEM((p.shape[1] // LANES, LANES, p.shape[0]), p.dtype) for p, *_ in parts],
            pltpu.SemaphoreType.DMA((count, max(steps))),
            pltpu.SemaphoreType.DMA((count, max(steps))),
        ],
        input_output_aliases={} if fresh else {count: 0, count + 1: 1},
        compiler_params=pltpu.CompilerParams(vmem_limit_bytes=32 * 2**20),
        cost_estimate=pl.CostEstimate(flops=0, bytes_accessed=moved, transcendentals=0),
    )(*operands)


def doubled(x, axis, pairs, high):
    other = lax.ppermute(x, axis, pairs)
    return jnp.where(high, jnp.concatenate([other, x]), jnp.concatenate([x, other]))


def gathered_gain(gain):
    length = gain.shape[0]
    y, xl, cols = (lax.axis_index(axis) for axis in ("y", "xl", "cols"))
    x_hi = (cols >> 1) & 1
    x = gain[None]
    for bit in (1, 4, 8):
        pairs = [(i, i ^ bit) for i in range(16)]
        x = doubled(x, "cols", pairs, (cols & bit) != 0)
    pairs = [(i, i ^ 18) for i in range(32)]
    x = doubled(x, ("xl", "cols"), pairs, x_hi == 1)
    index = jnp.arange(4)[:, None, None]
    mine = jnp.broadcast_to(x[None], (4, *x.shape))
    for shift in (1, 2, 3):
        part = lax.ppermute(x, "y", [(i, (i + shift) % 4) for i in range(4)])
        mine = jnp.where(index == (y - shift) % 4, part[None], mine)
    other = lax.ppermute(mine, "xl", SWAP)
    mine, other = (v.reshape(4, 1, 2, 2, 2, 2, length) for v in (mine, other))
    both = jnp.arange(2)
    own = (both[:, None] ^ both[None, :] ^ xl ^ x_hi) == 0
    x = jnp.where(own.reshape(1, 2, 2, 1, 1, 1, 1), mine, other)
    return x.transpose(0, 1, 3, 4, 2, 5, 6).reshape(-1)


def per_device(train_gate, low_gate, high_gate, train_up, low_up, high_up, norm_train, norm_step):
    rows, width = train_gate.shape

    def up(v):
        return lax.ppermute(v, "y", UP)

    def down(v):
        return lax.ppermute(v, "y", DOWN)

    def across(v):
        return lax.ppermute(v, "xl", SWAP)

    low_g, low_u = low_gate.T, low_up.T
    raw_g_x, raw_g_m, raw_u_p = across(train_gate), up(train_gate), down(train_up)
    low_g_x, low_g_m, low_u_p = across(low_g), up(low_g), down(low_u)
    g = merged(train_gate, low_g, high_gate)
    u = merged(train_up, low_u, high_up)
    gain = (norm_train + norm_step).astype(jnp.bfloat16)

    g_m = merged(raw_g_m, low_g_m, high_gate)
    g_x = merged(raw_g_x, low_g_x, high_gate)
    u_p = merged(raw_u_p, low_u_p, high_up)
    u_m, u_x, g_p = up(u), across(u), down(g)
    g_f, cg_p, cu_p = up(g_m), down(g_x), across(u_p)
    first, near, mid, late = width * 2 // 7, width * 4 // 7, width * 5 // 7, width * 6 // 7
    cu_m0, cu_m1, cu_m2 = (across(u_m[:, :near]), across(u_m[:, near:mid]), across(u_m[:, mid:]))
    cg_m, u_f = up(g_x), down(u_p)
    cg_f0, cg_f4, cg_f1 = (
        across(g_f[:, :first]), across(g_f[:, first:near]), across(g_f[LANES:, near:mid])
    )
    cg_f2, cg_f3 = down(cg_p[:, mid:]), down(cg_p[:LANES, near:mid])
    cu_f2, cu_f3 = down(cu_p[:, mid:late]), down(cu_p[:, late:])
    cu_f4 = down(cu_p[:LANES, near:mid])
    cu_f0, cu_f1 = up(cu_m0), up(cu_m1[LANES:])

    out = jax.ShapeDtypeStruct((width, rows * 8), jnp.bfloat16)
    outs = place((out, out), [(g, 0, 0, 0, 0), (u, 1, 0, 0, 0)])
    outs = place(outs, [(g_m, 0, 0, 3, 0), (g_x, 0, 0, 0, 1), (u_p, 1, 0, 1, 0)])
    outs = place(outs, [(u_m, 1, 0, 3, 0), (u_x, 1, 0, 0, 1), (g_p, 0, 0, 1, 0)])
    outs = place(outs, [(g_f, 0, 0, 2, 0), (cg_p, 0, 0, 1, 1), (cu_p, 1, 0, 1, 1)])
    outs = place(
        outs,
        [
            (cu_m0, 1, 0, 3, 1),
            (cu_m1, 1, near, 3, 1),
            (cu_m2, 1, mid, 3, 1),
            (cg_m, 0, 0, 3, 1),
            (u_f, 1, 0, 2, 0),
        ],
    )
    outs = place(outs, [(cg_f2, 0, mid, 2, 1), (cg_f3, 0, near, 2, 1), (cu_f4, 1, near, 2, 1), (cg_f0, 0, 0, 2, 1)], held=True)
    outs = place(
        outs, [(cg_f4, 0, first, 2, 1), (cu_f0, 1, 0, 2, 1), (cu_f2, 1, mid, 2, 1)], held=True
    )
    outs = place(
        outs,
        [(cg_f1, 0, near, 2, 1, LANES), (cu_f1, 1, near, 2, 1, LANES), (cu_f3, 1, late, 2, 1)],
        held=True,
    )
    return (*outs, gathered_gain(gain))


def solution(mesh):
    finer = Mesh(mesh.devices.reshape(4, 2, mesh.shape["cols"]), ("y", "xl", "cols"))
    shard, every = ("y", "xl"), ("y", "xl", "cols")
    return jax.shard_map(
        per_device,
        mesh=finer,
        in_specs=(
            P(shard, "cols"),
            P(shard, None),
            P(None, "cols"),
            P(shard, "cols"),
            P(shard, None),
            P(None, "cols"),
            P(every),
            P(every),
        ),
        out_specs=(P("cols", None), P("cols", None), P()),
        check_vma=False,
    )
```
